8 devices in a mesh: data: 1 (over z), cp: 2 (over y), tp: 4 (over x, core).
Axes of the slice: x: 2, y: 2, z: 1, core: 2. Of those that a mesh axis runs over, the one named last changes fastest.
Arguments:
- act_in: bfloat16 [2, 2048, 4096], P(None, ('data', 'cp', 'tp'))
- route_ids: int32 [2, 2048, 2], P(None, ('data', 'cp', 'tp'))
- route_gates: float32 [2, 2048, 2], P(None, ('data', 'cp', 'tp'))
- w_query: bfloat16 [4096, 64, 128], P(None, 'tp')
- w_key: bfloat16 [4096, 4, 128], P(None, 'tp')
- w_value: bfloat16 [4096, 4, 128], P(None, 'tp')
- w_out: bfloat16 [64, 128, 4096], P('tp')
- w_gate: bfloat16 [8, 4096, 1536], P(('cp', 'tp'))
- w_up: bfloat16 [8, 4096, 1536], P(('cp', 'tp'))
- w_down: bfloat16 [8, 1536, 4096], P(('cp', 'tp'))
Outputs:
- output: bfloat16 [2, 2048, 4096], P(None, ('data', 'cp', 'tp'))
All inputs are finite; a program needn't handle non-finite values.
Results may differ from the reference program's by a relative error of at most 0.00591.
Values are sent between devices in bfloat16 or wider.
A program may use at most 1 GiB of HBM per device.

```python
import math
import jax
import jax.numpy as jnp
from jax import lax

HIDDEN = 4096
EXPERT_FF = 1536
Q_HEADS = 64
KV_HEADS = 4
HEAD_DIM = 128
CP_SIZE = 2
TP_SIZE = 4
TOKENS_DEV = 256
MICRO_BATCHES = 2

EXPERTS = CP_SIZE * TP_SIZE
SEQ_LEN = TOKENS_DEV * EXPERTS
PIECE_LEN = SEQ_LEN // (2 * CP_SIZE)
CAPACITY = (4 * TOKENS_DEV) // EXPERTS
EXPERT_ROWS = CAPACITY * EXPERTS
GROUP_SIZE = Q_HEADS // KV_HEADS
SCORE_SHARP = math.sqrt(0.75 * math.log(SEQ_LEN))


def draw_routing(base_key):
    half_cap = CAPACITY // 2

    def one_source(src_key):
        k_perm, k_delta, k_tok, k_swap = jax.random.split(src_key, 4)
        expert_perm = jax.random.permutation(k_perm, EXPERTS)
        deltas = jax.random.randint(k_delta, (EXPERTS // 2,), 0, half_cap + 1).at[0].set(half_cap)
        pair_counts = jnp.stack([half_cap + deltas, half_cap - deltas], axis=1).reshape(EXPERTS)
        counts = jnp.zeros((EXPERTS,), jnp.int32).at[expert_perm].set(pair_counts)
        count_ends = jnp.cumsum(counts)
        labels = jnp.sum((jnp.arange(2 * TOKENS_DEV)[:, None] >= count_ends[None, :]).astype(jnp.int32), axis=1)
        id_pairs = jnp.stack([labels[:TOKENS_DEV], labels[TOKENS_DEV:]], axis=1)
        id_pairs = id_pairs[jax.random.permutation(k_tok, TOKENS_DEV)]
        swap_flag = jax.random.randint(k_swap, (TOKENS_DEV, 1), 0, 2)
        return jnp.where(swap_flag == 1, id_pairs[:, ::-1], id_pairs).astype(jnp.int32)

    return jax.vmap(one_source)(jax.random.split(base_key, EXPERTS)).reshape(SEQ_LEN, 2)


def normal_weight(weight_key, arr_shape, w_scale):
    return (jax.random.normal(weight_key, arr_shape, jnp.float32) * w_scale).astype(jnp.bfloat16)


def expert_stack(weight_key, arr_shape, w_scale):
    return lax.map(lambda one_key: normal_weight(one_key, arr_shape, w_scale), jax.random.split(weight_key, EXPERTS))


def setup_inputs(seed: int = 0, part: int = 0) -> dict:
    part_key = jax.random.fold_in(jax.random.key(seed), part)
    k_act, k_route, k_gate = jax.random.split(part_key, 3)
    shared = jax.random.split(jax.random.key(seed + 1), 7)
    act_in = jax.random.normal(k_act, (MICRO_BATCHES, SEQ_LEN, HIDDEN), jnp.float32).astype(jnp.bfloat16)
    route_ids = jax.vmap(draw_routing)(jax.random.split(k_route, MICRO_BATCHES))
    route_gates = jax.random.uniform(k_gate, (MICRO_BATCHES, SEQ_LEN, 2), jnp.float32, 0.3, 0.7)
    return {
        'act_in': act_in,
        'route_ids': route_ids,
        'route_gates': route_gates,
        'w_query': normal_weight(shared[0], (HIDDEN, Q_HEADS, HEAD_DIM), SCORE_SHARP / math.sqrt(HIDDEN)),
        'w_key': normal_weight(shared[1], (HIDDEN, KV_HEADS, HEAD_DIM), 1.0 / math.sqrt(HIDDEN)),
        'w_value': normal_weight(shared[2], (HIDDEN, KV_HEADS, HEAD_DIM), 1.0 / math.sqrt(HIDDEN)),
        'w_out': normal_weight(shared[3], (Q_HEADS, HEAD_DIM, HIDDEN), 1.0 / math.sqrt(Q_HEADS * HEAD_DIM)),
        'w_gate': expert_stack(shared[4], (HIDDEN, EXPERT_FF), 1.0 / math.sqrt(HIDDEN)),
        'w_up': expert_stack(shared[5], (HIDDEN, EXPERT_FF), 1.0 / math.sqrt(HIDDEN)),
        'w_down': expert_stack(shared[6], (EXPERT_FF, HIDDEN), 1.0 / math.sqrt(EXPERT_FF)),
    }


def token_positions():
    row_ix = jnp.arange(SEQ_LEN)
    owner_ix = row_ix // (2 * PIECE_LEN)
    inner_ix = row_ix % (2 * PIECE_LEN)
    return jnp.where(inner_ix < PIECE_LEN, owner_ix * PIECE_LEN + inner_ix, (2 * CP_SIZE - 1 - owner_ix) * PIECE_LEN + inner_ix - PIECE_LEN)


def attention_block(seq_in, w_query, w_key, w_value, w_out):
    query_rows = jnp.dot(seq_in, w_query.reshape(HIDDEN, Q_HEADS * HEAD_DIM), preferred_element_type=jnp.float32).astype(jnp.bfloat16)
    key_rows = jnp.dot(seq_in, w_key.reshape(HIDDEN, KV_HEADS * HEAD_DIM), preferred_element_type=jnp.float32).astype(jnp.bfloat16)
    value_rows = jnp.dot(seq_in, w_value.reshape(HIDDEN, KV_HEADS * HEAD_DIM), preferred_element_type=jnp.float32).astype(jnp.bfloat16)
    key_rows = key_rows.astype(jnp.float32).reshape(SEQ_LEN, KV_HEADS, HEAD_DIM)
    value_rows = value_rows.astype(jnp.float32).reshape(SEQ_LEN, KV_HEADS, HEAD_DIM)
    positions = token_positions()
    query_blocks = query_rows.reshape(EXPERTS, TOKENS_DEV, KV_HEADS, GROUP_SIZE, HEAD_DIM)
    pos_blocks = positions.reshape(EXPERTS, TOKENS_DEV)

    def one_block(block_args):
        q_block, q_pos = block_args
        scores = jnp.einsum('qhgd,khd->hgqk', q_block.astype(jnp.float32), key_rows) * HEAD_DIM ** -0.5
        scores = jnp.where(positions[None, :] <= q_pos[:, None], scores, -jnp.inf)
        row_peak = jnp.max(scores, axis=-1, keepdims=True)
        exp_scores = jnp.exp(scores - row_peak)
        row_sum = jnp.sum(exp_scores, axis=-1)
        weighted = jnp.einsum('hgqk,khd->qhgd', exp_scores.astype(jnp.bfloat16).astype(jnp.float32), value_rows)
        weighted = weighted / jnp.transpose(row_sum, (2, 0, 1))[..., None]
        return weighted.astype(jnp.bfloat16).reshape(TOKENS_DEV, Q_HEADS * HEAD_DIM)

    attn_rows = lax.map(one_block, (query_blocks, pos_blocks)).reshape(SEQ_LEN, Q_HEADS * HEAD_DIM)
    attn_sum = jnp.dot(attn_rows, w_out.reshape(Q_HEADS * HEAD_DIM, HIDDEN), preferred_element_type=jnp.float32)
    return (seq_in.astype(jnp.float32) + attn_sum).astype(jnp.bfloat16)


def expert_block(mid_rows, seq_ids, seq_gates, w_gate, w_up, w_down):
    choice_expert = seq_ids.reshape(2 * SEQ_LEN)
    choice_token = jnp.arange(2 * SEQ_LEN) // 2
    sort_ix = jnp.argsort(choice_expert, stable=True)
    counts = jnp.sum((choice_expert[None, :] == jnp.arange(EXPERTS)[:, None]).astype(jnp.int32), axis=1)
    starts = jnp.cumsum(counts) - counts
    sorted_token = jnp.concatenate([choice_token[sort_ix], jnp.zeros((EXPERT_ROWS,), choice_token.dtype)])

    def one_expert(expert_id):
        token_ids = lax.dynamic_slice(sorted_token, (starts[expert_id],), (EXPERT_ROWS,))
        expert_in = mid_rows[token_ids]
        gate_act = jnp.dot(expert_in, w_gate[expert_id], preferred_element_type=jnp.float32)
        up_act = jnp.dot(expert_in, w_up[expert_id], preferred_element_type=jnp.float32)
        mixed_act = (jax.nn.silu(gate_act) * up_act).astype(jnp.bfloat16)
        return jnp.dot(mixed_act, w_down[expert_id], preferred_element_type=jnp.float32).astype(jnp.bfloat16)

    expert_out = lax.map(one_expert, jnp.arange(EXPERTS)).reshape(EXPERTS * EXPERT_ROWS, HIDDEN)
    sorted_expert = choice_expert[sort_ix]
    slot_rank = jnp.arange(2 * SEQ_LEN) - starts[sorted_expert]
    z_sorted = expert_out[sorted_expert * EXPERT_ROWS + slot_rank]
    z_choice = z_sorted[jnp.argsort(sort_ix)].reshape(SEQ_LEN, 2, HIDDEN)
    mixed_sum = jnp.sum(seq_gates[:, :, None] * z_choice.astype(jnp.float32), axis=1)
    return (mid_rows.astype(jnp.float32) + mixed_sum).astype(jnp.bfloat16)


def reference(act_in, route_ids, route_gates, w_query, w_key, w_value, w_out, w_gate, w_up, w_down):
    def one_sequence(seq_args):
        seq_in, seq_ids, seq_gates = seq_args
        mid_rows = attention_block(seq_in, w_query, w_key, w_value, w_out)
        return expert_block(mid_rows, seq_ids, seq_gates, w_gate, w_up, w_down)

    return lax.map(one_sequence, (act_in, route_ids, route_gates))
```

```python
import functools
import math
import jax
import jax.numpy as jnp
from jax import lax
from jax.experimental import pallas as pl
from jax.experimental.pallas import tpu as pltpu
from jax.sharding import PartitionSpec as P

F32 = jnp.float32
BF16 = jnp.bfloat16


def attend_kernel(cp_ref, q_ref, own_ref, other_ref, o_ref, kt_own, kt_other, *, piece, head_dim):
    tile = piece // 2
    exp_scale = (head_dim ** -0.5) * math.log2(math.e)

    @pl.when(pl.program_id(0) == 0)
    def _():
        kt_own[...] = own_ref[:, :head_dim].T
        kt_other[...] = other_ref[:, :head_dim].T

    row_ix = lax.broadcasted_iota(jnp.int32, (tile, tile), 0)
    col_ix = lax.broadcasted_iota(jnp.int32, (tile, tile), 1)

    def one_tile(q_start, full_parts, diag_start):
        q_rows = q_ref[q_start:q_start + tile, :]
        scores, values = [], []
        for k_t, kv, start, size in full_parts:
            scores.append(jnp.dot(q_rows, k_t[:, start:start + size], preferred_element_type=F32))
            values.append((kv, start, size))
        diag = jnp.dot(q_rows, kt_own[:, diag_start:diag_start + tile], preferred_element_type=F32)
        scores.append(jnp.where(col_ix <= row_ix, diag, -jnp.inf))
        values.append((own_ref, diag_start, tile))
        peak = jnp.max(scores[0], axis=-1, keepdims=True)
        for part in scores[1:]:
            peak = jnp.maximum(peak, jnp.max(part, axis=-1, keepdims=True))
        peak = peak * exp_scale
        total = jnp.zeros((tile, 1), F32)
        acc = jnp.zeros((tile, head_dim), F32)
        for part, (kv, start, size) in zip(scores, values):
            weights = jnp.exp2(part * exp_scale - peak)
            total = total + jnp.sum(weights, axis=-1, keepdims=True)
            acc = acc + jnp.dot(weights.astype(BF16), kv[start:start + size, head_dim:], preferred_element_type=F32)
        o_ref[q_start:q_start + tile, :] = (acc / total).astype(BF16)

    def piece_tiles(q_start, full_parts):
        one_tile(q_start, full_parts, q_start)
        one_tile(q_start + tile, full_parts + [(kt_own, own_ref, q_start, tile)], q_start + tile)

    own_low = (kt_own, own_ref, 0, piece)
    other_low = (kt_other, other_ref, 0, piece)
    other_high = (kt_other, other_ref, piece, piece)

    @pl.when(cp_ref[0] == 0)
    def _():
        piece_tiles(0, [])
        piece_tiles(piece, [own_low, other_low, other_high])

    @pl.when(cp_ref[0] == 1)
    def _():
        piece_tiles(0, [other_low])
        piece_tiles(piece, [own_low, other_low])


def attend(q_rows, kv_own, kv_other, cp_rank, head_dim):
    rows, width = q_rows.shape
    heads = width // head_dim
    piece = rows // 2
    kv_spec = pl.BlockSpec((rows, 2 * head_dim), lambda h, s: (0, 0))
    head_spec = pl.BlockSpec((rows, head_dim), lambda h, s: (0, h))
    work = 5 * piece * piece * heads
    return pl.pallas_call(
        functools.partial(attend_kernel, piece=piece, head_dim=head_dim),
        out_shape=jax.ShapeDtypeStruct((rows, width), BF16),
        grid_spec=pltpu.PrefetchScalarGridSpec(
            num_scalar_prefetch=1,
            grid=(heads,),
            in_specs=[head_spec, kv_spec, kv_spec],
            out_specs=head_spec,
            scratch_shapes=[pltpu.VMEM((head_dim, rows), BF16), pltpu.VMEM((head_dim, rows), BF16)],
        ),
        compiler_params=pltpu.CompilerParams(dimension_semantics=('arbitrary',)),
        cost_estimate=pl.CostEstimate(flops=4 * work * head_dim * 2, bytes_accessed=4 * rows * width + 8 * rows * head_dim, transcendentals=work),
        name='attend',
    )(cp_rank.reshape(1), q_rows, kv_own, kv_other)


def rank_in_expert(token_hits):
    tokens = token_hits.shape[-2]
    earlier = (jnp.arange(tokens)[None, :] < jnp.arange(tokens)[:, None]).astype(BF16)
    return jnp.einsum('ts,...se->...te', earlier, token_hits.astype(BF16), preferred_element_type=F32).astype(jnp.int32)


def solution(mesh):
    cp_size = mesh.shape['cp']
    tp_size = mesh.shape['tp']
    experts = cp_size * tp_size
    row_spec = P(None, ('data', 'cp', 'tp'), None)
    head_spec = P(None, 'tp', None)
    out_spec = P('tp', None, None)
    expert_spec = P(('cp', 'tp'), None, None)
    both = ('cp', 'tp')

    def device_step(act_in, route_ids, route_gates, w_query, w_key, w_value, w_out, w_gate, w_up, w_down):
        n_seq, tokens, hidden = act_in.shape
        head_dim = w_query.shape[2]
        capacity = (4 * tokens) // experts
        cp_rank = lax.axis_index('cp')
        my_expert = cp_rank * tp_size + lax.axis_index('tp')
        w_q = w_query.reshape(hidden, -1)
        w_kv = jnp.concatenate([w_key.reshape(hidden, -1), w_value.reshape(hidden, -1)], axis=1)
        w_o = w_out.reshape(-1, hidden)

        ids_all = lax.all_gather(route_ids, both, axis=0)
        hit_here = jnp.any(ids_all == my_expert, axis=-1)
        rank_here = rank_in_expert(hit_here[..., None])[..., 0]
        slot_token = jnp.where(hit_here, rank_here, -1)[:, :, None, :] == jnp.arange(capacity)[:, None]
        pick_in = slot_token.astype(BF16)

        hits = route_ids[..., None] == jnp.arange(experts)
        ranks = rank_in_expert(jnp.any(hits, axis=2))
        choice_rank = jnp.sum(hits * ranks[:, :, None, :], axis=-1)
        choice_slot = route_ids * capacity + choice_rank
        choice_slot = jnp.swapaxes(choice_slot, 1, 2).reshape(n_seq, 2 * tokens)
        pick_back = (choice_slot[..., None] == jnp.arange(experts * capacity)).astype(BF16)

        swap = [(i, i ^ 1) for i in range(cp_size)]
        outs = []
        for seq in range(n_seq):
            x_own = act_in[seq]
            x_half = lax.all_gather(x_own, 'tp', axis=0, tiled=True)
            if seq == 0:
                x_half, pick_in, pick_back = lax.optimization_barrier((x_half, pick_in, pick_back))
            kv_own = jnp.dot(x_half, w_kv, preferred_element_type=F32).astype(BF16)
            kv_other = lax.ppermute(kv_own, 'cp', swap)
            q_rows = jnp.dot(x_half, w_q, preferred_element_type=F32).astype(BF16)
            attn_rows = attend(q_rows, kv_own, kv_other, cp_rank, head_dim)
            partial = jnp.dot(attn_rows, w_o, preferred_element_type=F32)
            attn_sum = lax.psum_scatter(partial, 'tp', scatter_dimension=0, tiled=True)
            if seq > 0:
                x_own, mid_rows = lax.optimization_barrier((x_own, mid_rows))
            mid_rows = (x_own.astype(F32) + attn_sum).astype(BF16)
            mid_all = lax.all_gather(mid_rows, both, axis=0)
            expert_in = jnp.einsum('dst,dth->dsh', pick_in[:, seq], mid_all, preferred_element_type=F32).astype(BF16)
            expert_in = expert_in.reshape(experts * capacity, hidden)
            gate_act = jnp.dot(expert_in, w_gate[0], preferred_element_type=F32)
            up_act = jnp.dot(expert_in, w_up[0], preferred_element_type=F32)
            mixed_act = (jax.nn.silu(gate_act) * up_act).astype(BF16)
            expert_out = jnp.dot(mixed_act, w_down[0], preferred_element_type=F32).astype(BF16)
            back = lax.all_to_all(expert_out.reshape(experts, capacity, hidden), both, 0, 0, tiled=True)
            back = back.reshape(experts * capacity, hidden)
            picked = jnp.dot(pick_back[seq], back, preferred_element_type=F32).astype(BF16)
            combined = route_gates[seq, :, 0:1] * picked[:tokens].astype(F32) + route_gates[seq, :, 1:2] * picked[tokens:].astype(F32)
            outs.append((mid_rows.astype(F32) + combined).astype(BF16))
        return jnp.stack(outs)

    return jax.shard_map(device_step, mesh=mesh, in_specs=(row_spec, row_spec, row_spec, head_spec, head_spec, head_spec, out_spec, expert_spec, expert_spec, expert_spec), out_specs=row_spec, check_vma=False)
```

```python
import functools
import math
import jax
import jax.numpy as jnp
from jax import lax
from jax.experimental import pallas as pl
from jax.experimental.pallas import tpu as pltpu
from jax.sharding import PartitionSpec as P

F32 = jnp.float32
BF16 = jnp.bfloat16


def attend_kernel(ids_ref, q_ref, *refs, n_pieces, piece, head_dim):
    kv_refs, (o_ref, k_scr, v_scr) = refs[:n_pieces], refs[n_pieces:]
    tile = piece // 2
    exp_scale = (head_dim ** -0.5) * math.log2(math.e)

    @pl.when(pl.program_id(0) == 0)
    def _():
        for i, kv_ref in enumerate(kv_refs):
            where = ids_ref[1 + i]
            k_scr[where] = kv_ref[:, :head_dim].T
            v_scr[where] = kv_ref[:, head_dim:]

    row_ix = lax.broadcasted_iota(jnp.int32, (tile, tile), 0)
    col_ix = lax.broadcasted_iota(jnp.int32, (tile, tile), 1)

    def one_tile(half, piece_id):
        q_rows = q_ref[half * tile:(half + 1) * tile, :]
        parts = [(p, 0, piece) for p in range(piece_id)]
        if half == 1:
            parts.append((piece_id, 0, tile))
        parts.append((piece_id, half * tile, tile))
        scores = [jnp.dot(q_rows, k_scr[p, :, start:start + size], preferred_element_type=F32) for p, start, size in parts]
        scores[-1] = jnp.where(col_ix <= row_ix, scores[-1], -jnp.inf)
        peak = jnp.max(scores[0], axis=-1, keepdims=True)
        for part in scores[1:]:
            peak = jnp.maximum(peak, jnp.max(part, axis=-1, keepdims=True))
        peak = peak * exp_scale
        total = jnp.zeros((tile, 1), F32)
        acc = jnp.zeros((tile, head_dim), F32)
        for part, (p, start, size) in zip(scores, parts):
            weights = jnp.exp2(part * exp_scale - peak)
            total = total + jnp.sum(weights, axis=-1, keepdims=True)
            acc = acc + jnp.dot(weights.astype(BF16), v_scr[p, start:start + size, :], preferred_element_type=F32)
        o_ref[half * tile:(half + 1) * tile, :] = (acc / total).astype(BF16)

    for piece_id in range(n_pieces):
        @pl.when(ids_ref[0] == piece_id)
        def _():
            one_tile(0, piece_id)
            one_tile(1, piece_id)


def attend(q_rows, kv_list, ids, head_dim):
    piece, width = q_rows.shape
    heads = width // head_dim
    n_pieces = len(kv_list)
    kv_spec = pl.BlockSpec((piece, 2 * head_dim), lambda h, s: (0, 0))
    head_spec = pl.BlockSpec((piece, head_dim), lambda h, s: (0, h))
    work = 5 * piece * piece * heads // 2
    return pl.pallas_call(
        functools.partial(attend_kernel, n_pieces=n_pieces, piece=piece, head_dim=head_dim),
        out_shape=jax.ShapeDtypeStruct((piece, width), BF16),
        grid_spec=pltpu.PrefetchScalarGridSpec(
            num_scalar_prefetch=1,
            grid=(heads,),
            in_specs=[head_spec] + [kv_spec] * n_pieces,
            out_specs=head_spec,
            scratch_shapes=[pltpu.VMEM((n_pieces, head_dim, piece), BF16), pltpu.VMEM((n_pieces, piece, head_dim), BF16)],
        ),
        compiler_params=pltpu.CompilerParams(dimension_semantics=('arbitrary',)),
        cost_estimate=pl.CostEstimate(flops=4 * work * head_dim * 2, bytes_accessed=4 * piece * width + 4 * n_pieces * piece * head_dim, transcendentals=work),
        name='attend',
    )(ids, q_rows, *kv_list)


def combine_kernel(slot_ref, gate_ref, mid_ref, *refs, n_back, capacity, aliased):
    back_refs = refs[:n_back]
    out_ref, hot_scr, back_scr = refs[n_back + (1 if aliased else 0):]
    tokens = mid_ref.shape[0]

    @pl.when(pl.program_id(0) == 0)
    def _():
        slot_ix = lax.broadcasted_iota(jnp.int32, (2 * tokens, n_back * capacity), 1)
        hot_scr[...] = jnp.where(slot_ix == slot_ref[...], 1.0, 0.0).astype(BF16)

    for i in range(n_back):
        back_scr[i * capacity:(i + 1) * capacity, :] = back_refs[i][...]
    picked = jnp.dot(hot_scr[...], back_scr[...], preferred_element_type=F32)
    gated = gate_ref[:, 0:1] * picked[:tokens] + gate_ref[:, 1:2] * picked[tokens:]
    out_ref[0] = (mid_ref[...].astype(F32) + gated).astype(BF16)


def combine(seq, n_seq, slots, gates, mid_rows, back_list, out_prev):
    tokens, hidden = mid_rows.shape
    n_back = len(back_list)
    capacity = back_list[0].shape[0]
    width = 512
    aliased = out_prev is not None
    whole = lambda shape: pl.BlockSpec(shape, lambda i: (0, 0))
    column = lambda rows: pl.BlockSpec((rows, width), lambda i: (0, i))
    in_specs = [whole((2 * tokens, 1)), whole((tokens, 2)), column(tokens)] + [column(capacity)] * n_back
    args = [slots, gates, mid_rows] + list(back_list)
    if aliased:
        in_specs.append(pl.BlockSpec(memory_space=pl.ANY))
        args.append(out_prev)
    return pl.pallas_call(
        functools.partial(combine_kernel, n_back=n_back, capacity=capacity, aliased=aliased),
        out_shape=jax.ShapeDtypeStruct((n_seq, tokens, hidden), BF16),
        grid=(hidden // width,),
        in_specs=in_specs,
        out_specs=pl.BlockSpec((1, tokens, width), lambda i: (seq, 0, i)),
        scratch_shapes=[pltpu.VMEM((2 * tokens, n_back * capacity), BF16), pltpu.VMEM((n_back * capacity, width), BF16)],
        input_output_aliases={len(args) - 1: 0} if aliased else {},
        compiler_params=pltpu.CompilerParams(dimension_semantics=('arbitrary',)),
        cost_estimate=pl.CostEstimate(flops=4 * tokens * n_back * capacity * hidden, bytes_accessed=2 * hidden * (n_back * capacity + 2 * tokens), transcendentals=0),
        name='combine',
    )(*args)


def rank_in_expert(token_hits):
    tokens = token_hits.shape[-2]
    earlier = (jnp.arange(tokens)[None, :] < jnp.arange(tokens)[:, None]).astype(BF16)
    return jnp.einsum('ts,...se->...te', earlier, token_hits.astype(BF16), preferred_element_type=F32).astype(jnp.int32)


def solution(mesh):
    cp_size = mesh.shape['cp']
    tp_size = mesh.shape['tp']
    experts = cp_size * tp_size
    row_spec = P(None, ('data', 'cp', 'tp'), None)
    head_spec = P(None, 'tp', None)
    out_spec = P('tp', None, None)
    expert_spec = P(('cp', 'tp'), None, None)
    both = ('cp', 'tp')
    cores = [[0, 1], [2, 3]]

    def cross_x(rows):
        return lax.ppermute(rows, 'tp', [(t, t ^ 2) for t in range(tp_size)])

    def cross_y(rows):
        return lax.ppermute(rows, 'cp', [(c, c ^ 1) for c in range(cp_size)])

    def pair(rows):
        return lax.all_gather(rows, 'tp', axis=0, tiled=True, axis_index_groups=cores)

    def exchange(rows, k):
        return rows if k == 0 else lax.ppermute(rows, both, [(i, i ^ k) for i in range(experts)])

    def device_step(act_in, route_ids, route_gates, w_query, w_key, w_value, w_out, w_gate, w_up, w_down):
        n_seq, tokens, hidden = act_in.shape
        head_dim = w_query.shape[2]
        capacity = (4 * tokens) // experts
        cp_rank = lax.axis_index('cp')
        tp_rank = lax.axis_index('tp')
        x_rank, core = tp_rank // 2, tp_rank % 2
        me = cp_rank * tp_size + tp_rank
        w_q = w_query.reshape(hidden, -1)
        w_kv = jnp.concatenate([w_key.reshape(hidden, -1), w_value.reshape(hidden, -1)], axis=1)
        w_o = w_out.reshape(-1, hidden)

        piece_of = lambda c, x: jnp.where(x == 0, c, 2 * cp_size - 1 - c)
        piece_ids = [piece_of(cp_rank, x_rank), piece_of(cp_rank, 1 - x_rank), piece_of(1 - cp_rank, x_rank), piece_of(1 - cp_rank, 1 - x_rank)]
        ids_here = jnp.stack([piece_ids[0]] + piece_ids)
        ids_there = jnp.stack([piece_ids[1]] + piece_ids)

        def project(rows):
            kv = jnp.dot(rows, w_kv, preferred_element_type=F32).astype(BF16)
            return kv, jnp.dot(rows, w_q, preferred_element_type=F32).astype(BF16)

        def project_out(rows):
            part = jnp.dot(rows, w_o, preferred_element_type=F32)
            return lax.psum_scatter(part, 'tp', scatter_dimension=0, tiled=True, axis_index_groups=cores)

        ids_by = jnp.stack([route_ids, exchange(route_ids, 1)])
        ids_by = jnp.concatenate([ids_by, cross_x(ids_by)])
        ids_by = jnp.concatenate([ids_by, cross_y(ids_by)])

        hit_here = jnp.any(ids_by == me, axis=-1)
        rank_here = rank_in_expert(hit_here[..., None])[..., 0]
        slot_of = jnp.where(hit_here, rank_here, -1).reshape(experts // 2, 2, n_seq, tokens)
        slot_of = jnp.where(core == 0, slot_of, slot_of[:, ::-1])
        slot_of = jnp.swapaxes(slot_of, 1, 2).reshape(experts // 2, n_seq, 1, 2 * tokens)
        slot_ix = jnp.arange(2 * capacity)[:, None]
        same = jnp.arange(2 * tokens)[None, :] // tokens == (slot_ix // capacity ^ core)
        pick_in = ((slot_of == slot_ix % capacity) & same).astype(BF16)

        hits = route_ids[..., None] == jnp.arange(experts)
        ranks = rank_in_expert(jnp.any(hits, axis=2))
        choice_rank = jnp.sum(hits * ranks[:, :, None, :], axis=-1)
        choice_slot = (route_ids ^ me) * capacity + choice_rank
        choice_slot = jnp.swapaxes(choice_slot, 1, 2).reshape(n_seq, 2 * tokens, 1)

        mids, mids_x, mids_y = [], [], []
        for seq in range(n_seq):
            x_own = act_in[seq]
            x_over = cross_x(x_own)
            rows_here = pair(x_own)
            kv_here, q_here = project(rows_here)
            kv_y_here = cross_y(kv_here)
            rows_there = pair(x_over)
            kv_there, q_there = project(rows_there)
            kv_y_there = cross_y(kv_there)
            kv_list = [kv_here, kv_there, kv_y_here, kv_y_there]
            attn_there = attend(q_there, kv_list, ids_there, head_dim)
            sum_there = project_out(attn_there)
            attn_here = attend(q_here, kv_list, ids_here, head_dim)
            sum_over = cross_x(sum_there)
            sum_here = project_out(attn_here)
            if seq > 0:
                x_own, _ = lax.optimization_barrier((x_own, mids[-1]))
            mids.append((x_own.astype(F32) + (sum_here + sum_over)).astype(BF16))
            mids_x.append(cross_x(mids[-1]))
            mids_y.append(cross_y(mids[-1]))

        out = None
        for seq in range(n_seq):
            mid_diag = cross_y(mids_x[seq])
            rows_of = [mids[seq], mids_x[seq], mids_y[seq], mid_diag]
            backs = [None] * experts
            for group in ((1, 2), (3, 0)):
                picks = []
                for kc in group:
                    rows_two = pair(rows_of[kc])
                    picks.append(jnp.dot(pick_in[kc, seq], rows_two, preferred_element_type=F32).astype(BF16))
                expert_in = jnp.concatenate(picks, axis=0)
                gate_act = jnp.dot(expert_in, w_gate[0], preferred_element_type=F32)
                up_act = jnp.dot(expert_in, w_up[0], preferred_element_type=F32)
                mixed_act = (jax.nn.silu(gate_act) * up_act).astype(BF16)
                mixed_act = lax.optimization_barrier(mixed_act)
                expert_out = jnp.dot(mixed_act, w_down[0], preferred_element_type=F32).astype(BF16)
                for i, kc in enumerate(group):
                    for r in range(2):
                        start = (2 * i + r) * capacity
                        backs[2 * kc + r] = exchange(expert_out[start:start + capacity], 2 * kc + r)
            out = combine(seq, n_seq, choice_slot[seq], route_gates[seq], mids[seq], backs, out)
        return out

    return jax.shard_map(device_step, mesh=mesh, in_specs=(row_spec, row_spec, row_spec, head_spec, head_spec, head_spec, out_spec, expert_spec, expert_spec, expert_spec), out_specs=row_spec, check_vma=False)
```

```python
import functools
import math
import jax
import jax.numpy as jnp
from jax import lax
from jax.experimental import pallas as pl
from jax.experimental.pallas import tpu as pltpu
from jax.sharding import PartitionSpec as P

F32 = jnp.float32
BF16 = jnp.bfloat16


def attend_kernel(ids_ref, q_ref, *refs, n_pieces, piece, head_dim, heads_step):
    kv_refs, (o_ref, k_scr, v_scr) = refs[:n_pieces], refs[n_pieces:]
    tile = piece // 2
    exp_scale = (head_dim ** -0.5) * math.log2(math.e)

    @pl.when(pl.program_id(0) == 0)
    def _():
        for i, kv_ref in enumerate(kv_refs):
            where = ids_ref[1 + i]

            @pl.when(where <= ids_ref[0])
            def _():
                k_scr[where] = kv_ref[:, :head_dim].T
                v_scr[where] = kv_ref[:, head_dim:]

    row_ix = lax.broadcasted_iota(jnp.int32, (tile, tile), 0)
    col_ix = lax.broadcasted_iota(jnp.int32, (tile, tile), 1)

    def parts_of(half, piece_id):
        parts = [(p, 0, piece) for p in range(piece_id)]
        if half == 1:
            parts.append((piece_id, 0, tile))
        return parts + [(piece_id, half * tile, tile)]

    def scores_of(head, half, piece_id):
        q_rows = q_ref[half * tile:(half + 1) * tile, head * head_dim:(head + 1) * head_dim]
        scores = [jnp.dot(q_rows, k_scr[p, :, start:start + size], preferred_element_type=F32) for p, start, size in parts_of(half, piece_id)]
        scores[-1] = jnp.where(col_ix <= row_ix, scores[-1], -jnp.inf)
        return scores

    def finish(head, half, piece_id, scores):
        peak = jnp.max(scores[0], axis=-1, keepdims=True)
        for part in scores[1:]:
            peak = jnp.maximum(peak, jnp.max(part, axis=-1, keepdims=True))
        peak = peak * exp_scale
        total = jnp.zeros((tile, 1), F32)
        acc = jnp.zeros((tile, head_dim), F32)
        for part, (p, start, size) in zip(scores, parts_of(half, piece_id)):
            weights = jnp.exp2(part * exp_scale - peak)
            total = total + jnp.sum(weights, axis=-1, keepdims=True)
            acc = acc + jnp.dot(weights.astype(BF16), v_scr[p, start:start + size, :], preferred_element_type=F32)
        o_ref[half * tile:(half + 1) * tile, head * head_dim:(head + 1) * head_dim] = (acc / total).astype(BF16)

    tiles = [(head, half) for head in range(heads_step) for half in range(2)]
    for piece_id in range(n_pieces):
        @pl.when(ids_ref[0] == piece_id)
        def _():
            ahead = scores_of(*tiles[0], piece_id)
            for now, later in zip(tiles, tiles[1:] + [None]):
                scores = ahead
                if later is not None:
                    ahead = scores_of(*later, piece_id)
                finish(*now, piece_id, scores)


def attend(q_rows, kv_list, ids, head_dim):
    piece, width = q_rows.shape
    heads = width // head_dim
    heads_step = 2
    n_pieces = len(kv_list)
    kv_spec = pl.BlockSpec((piece, 2 * head_dim), lambda h, s: (0, 0))
    head_spec = pl.BlockSpec((piece, heads_step * head_dim), lambda h, s: (0, h))
    work = 5 * piece * piece * heads // 2
    return pl.pallas_call(
        functools.partial(attend_kernel, n_pieces=n_pieces, piece=piece, head_dim=head_dim, heads_step=heads_step),
        out_shape=jax.ShapeDtypeStruct((piece, width), BF16),
        grid_spec=pltpu.PrefetchScalarGridSpec(
            num_scalar_prefetch=1,
            grid=(heads // heads_step,),
            in_specs=[head_spec] + [kv_spec] * n_pieces,
            out_specs=head_spec,
            scratch_shapes=[pltpu.VMEM((n_pieces, head_dim, piece), BF16), pltpu.VMEM((n_pieces, piece, head_dim), BF16)],
        ),
        compiler_params=pltpu.CompilerParams(dimension_semantics=('arbitrary',)),
        cost_estimate=pl.CostEstimate(flops=4 * work * head_dim * 2, bytes_accessed=4 * piece * width + 4 * n_pieces * piece * head_dim, transcendentals=work),
        name='attend',
    )(ids, q_rows, *kv_list)


def combine_kernel(slot_ref, gate_ref, mid_ref, *refs, n_back, capacity, aliased):
    back_refs = refs[:n_back]
    out_ref, hot_scr, back_scr = refs[n_back + (1 if aliased else 0):]
    tokens = mid_ref.shape[0]

    @pl.when(pl.program_id(0) == 0)
    def _():
        slot_ix = lax.broadcasted_iota(jnp.int32, (2 * tokens, n_back * capacity), 1)
        hot_scr[...] = jnp.where(slot_ix == slot_ref[...], 1.0, 0.0).astype(BF16)

    for i in range(n_back):
        back_scr[i * capacity:(i + 1) * capacity, :] = back_refs[i][...]
    picked = jnp.dot(hot_scr[...], back_scr[...], preferred_element_type=F32)
    gated = gate_ref[:, 0:1] * picked[:tokens] + gate_ref[:, 1:2] * picked[tokens:]
    out_ref[0] = (mid_ref[...].astype(F32) + gated).astype(BF16)


def combine(seq, n_seq, slots, gates, mid_rows, back_list, out_prev):
    tokens, hidden = mid_rows.shape
    n_back = len(back_list)
    capacity = back_list[0].shape[0]
    width = 512
    aliased = out_prev is not None
    whole = lambda shape: pl.BlockSpec(shape, lambda i: (0, 0))
    column = lambda rows: pl.BlockSpec((rows, width), lambda i: (0, i))
    in_specs = [whole((2 * tokens, 1)), whole((tokens, 2)), column(tokens)] + [column(capacity)] * n_back
    args = [slots, gates, mid_rows] + list(back_list)
    if aliased:
        in_specs.append(pl.BlockSpec(memory_space=pl.ANY))
        args.append(out_prev)
    return pl.pallas_call(
        functools.partial(combine_kernel, n_back=n_back, capacity=capacity, aliased=aliased),
        out_shape=jax.ShapeDtypeStruct((n_seq, tokens, hidden), BF16),
        grid=(hidden // width,),
        in_specs=in_specs,
        out_specs=pl.BlockSpec((1, tokens, width), lambda i: (seq, 0, i)),
        scratch_shapes=[pltpu.VMEM((2 * tokens, n_back * capacity), BF16), pltpu.VMEM((n_back * capacity, width), BF16)],
        input_output_aliases={len(args) - 1: 0} if aliased else {},
        compiler_params=pltpu.CompilerParams(dimension_semantics=('arbitrary',)),
        cost_estimate=pl.CostEstimate(flops=4 * tokens * n_back * capacity * hidden, bytes_accessed=2 * hidden * (n_back * capacity + 2 * tokens), transcendentals=0),
        name='combine',
    )(*args)


def rank_in_expert(token_hits):
    tokens = token_hits.shape[-2]
    earlier = (jnp.arange(tokens)[None, :] < jnp.arange(tokens)[:, None]).astype(BF16)
    return jnp.einsum('ts,...se->...te', earlier, token_hits.astype(BF16), preferred_element_type=F32).astype(jnp.int32)


def solution(mesh):
    cp_size = mesh.shape['cp']
    tp_size = mesh.shape['tp']
    experts = cp_size * tp_size
    row_spec = P(None, ('data', 'cp', 'tp'), None)
    head_spec = P(None, 'tp', None)
    out_spec = P('tp', None, None)
    expert_spec = P(('cp', 'tp'), None, None)
    both = ('cp', 'tp')
    cores = [[0, 1], [2, 3]]

    def cross_x(rows):
        return lax.ppermute(rows, 'tp', [(t, t ^ 2) for t in range(tp_size)])

    def cross_y(rows):
        return lax.ppermute(rows, 'cp', [(c, c ^ 1) for c in range(cp_size)])

    def pair(rows):
        return lax.all_gather(rows, 'tp', axis=0, tiled=True, axis_index_groups=cores)

    def exchange(rows, k):
        return rows if k == 0 else lax.ppermute(rows, both, [(i, i ^ k) for i in range(experts)])

    def device_step(act_in, route_ids, route_gates, w_query, w_key, w_value, w_out, w_gate, w_up, w_down):
        n_seq, tokens, hidden = act_in.shape
        head_dim = w_query.shape[2]
        capacity = (4 * tokens) // experts
        cp_rank = lax.axis_index('cp')
        tp_rank = lax.axis_index('tp')
        x_rank, core = tp_rank // 2, tp_rank % 2
        me = cp_rank * tp_size + tp_rank
        w_q = w_query.reshape(hidden, -1)
        w_kv = jnp.concatenate([w_key.reshape(hidden, -1), w_value.reshape(hidden, -1)], axis=1)
        w_o = w_out.reshape(-1, hidden)

        piece_of = lambda c, x: jnp.where(x == 0, c, 2 * cp_size - 1 - c)
        piece_ids = [piece_of(cp_rank, x_rank), piece_of(cp_rank, 1 - x_rank), piece_of(1 - cp_rank, x_rank), piece_of(1 - cp_rank, 1 - x_rank)]
        ids_here = jnp.stack([piece_ids[0]] + piece_ids)
        ids_there = jnp.stack([piece_ids[1]] + piece_ids)

        def project(rows):
            kv = jnp.dot(rows, w_kv, preferred_element_type=F32).astype(BF16)
            return kv, jnp.dot(rows, w_q, preferred_element_type=F32).astype(BF16)

        def project_out(rows):
            part = jnp.dot(rows, w_o, preferred_element_type=F32)
            return lax.psum_scatter(part, 'tp', scatter_dimension=0, tiled=True, axis_index_groups=cores)

        ids_by = jnp.stack([route_ids, exchange(route_ids, 1)])
        ids_by = jnp.concatenate([ids_by, cross_x(ids_by)])
        ids_by = jnp.concatenate([ids_by, cross_y(ids_by)])

        hit_here = jnp.any(ids_by == me, axis=-1)
        rank_here = rank_in_expert(hit_here[..., None])[..., 0]
        slot_of = jnp.where(hit_here, rank_here, -1).reshape(experts // 2, 2, n_seq, tokens)
        slot_of = jnp.where(core == 0, slot_of, slot_of[:, ::-1])
        slot_of = jnp.swapaxes(slot_of, 1, 2).reshape(experts // 2, n_seq, 1, 2 * tokens)
        slot_ix = jnp.arange(2 * capacity)[:, None]
        same = jnp.arange(2 * tokens)[None, :] // tokens == (slot_ix // capacity ^ core)
        pick_in = ((slot_of == slot_ix % capacity) & same).astype(BF16)

        hits = route_ids[..., None] == jnp.arange(experts)
        ranks = rank_in_expert(jnp.any(hits, axis=2))
        choice_rank = jnp.sum(hits * ranks[:, :, None, :], axis=-1)
        choice_slot = (route_ids ^ me) * capacity + choice_rank
        choice_slot = jnp.swapaxes(choice_slot, 1, 2).reshape(n_seq, 2 * tokens, 1)

        mids, mids_x, mids_y = [], [], []
        for seq in range(n_seq):
            x_own = act_in[seq]
            x_over = cross_x(x_own)
            rows_here = pair(x_own)
            kv_here, q_here = project(rows_here)
            kv_y_here = cross_y(kv_here)
            rows_there = pair(x_over)
            kv_there, q_there = project(rows_there)
            kv_y_there = cross_y(kv_there)
            kv_list = [kv_here, kv_there, kv_y_here, kv_y_there]
            attn_there = attend(q_there, kv_list, ids_there, head_dim)
            sum_there = project_out(attn_there)
            attn_here = attend(q_here, kv_list, ids_here, head_dim)
            sum_over = cross_x(sum_there)
            sum_here = project_out(attn_here)
            if seq > 0:
                x_own, _ = lax.optimization_barrier((x_own, mids[-1]))
            mids.append((x_own.astype(F32) + (sum_here + sum_over)).astype(BF16))
            mids_x.append(cross_x(mids[-1]))
            mids_y.append(cross_y(mids[-1]))

        out = None
        for seq in range(n_seq):
            mid_diag = cross_y(mids_x[seq])
            rows_of = [mids[seq], mids_x[seq], mids_y[seq], mid_diag]
            backs = [None] * experts
            for group in ((1, 2), (3, 0)):
                picks = []
                for kc in group:
                    rows_two = pair(rows_of[kc])
                    picks.append(jnp.dot(pick_in[kc, seq], rows_two, preferred_element_type=F32).astype(BF16))
                expert_in = jnp.concatenate(picks, axis=0)
                gate_act = jnp.dot(expert_in, w_gate[0], preferred_element_type=F32)
                up_act = jnp.dot(expert_in, w_up[0], preferred_element_type=F32)
                mixed_act = (jax.nn.silu(gate_act) * up_act).astype(BF16)
                mixed_act = lax.optimization_barrier(mixed_act)
                expert_out = jnp.dot(mixed_act, w_down[0], preferred_element_type=F32).astype(BF16)
                for i, kc in enumerate(group):
                    for r in range(2):
                        start = (2 * i + r) * capacity
                        backs[2 * kc + r] = exchange(expert_out[start:start + capacity], 2 * kc + r)
            out = combine(seq, n_seq, choice_slot[seq], route_gates[seq], mids[seq], backs, out)
        return out

    return jax.shard_map(device_step, mesh=mesh, in_specs=(row_spec, row_spec, row_spec, head_spec, head_spec, head_spec, out_spec, expert_spec, expert_spec, expert_spec), out_specs=row_spec, check_vma=False)
```

```python
import functools
import math
import jax
import jax.numpy as jnp
from jax import lax
from jax.experimental import pallas as pl
from jax.experimental.pallas import tpu as pltpu
from jax.sharding import PartitionSpec as P

F32 = jnp.float32
BF16 = jnp.bfloat16


def attend_kernel(ids_ref, q_ref, *refs, n_pieces, piece, head_dim, heads_step):
    kv_refs, (o_ref, k_scr, v_scr) = refs[:n_pieces], refs[n_pieces:]
    tile = piece // 2
    exp_scale = (head_dim ** -0.5) * math.log2(math.e)

    @pl.when(pl.program_id(0) == 0)
    def _():
        for i, kv_ref in enumerate(kv_refs):
            where = ids_ref[1 + i]

            @pl.when(where <= ids_ref[0])
            def _():
                k_scr[where] = kv_ref[:, :head_dim].T
                v_scr[where] = kv_ref[:, head_dim:]

    row_ix = lax.broadcasted_iota(jnp.int32, (tile, tile), 0)
    col_ix = lax.broadcasted_iota(jnp.int32, (tile, tile), 1)

    def parts_of(half, piece_id):
        parts = [(p, 0, piece) for p in range(piece_id)]
        if half == 1:
            parts.append((piece_id, 0, tile))
        return parts + [(piece_id, half * tile, tile)]

    def scores_of(head, half, piece_id):
        q_rows = q_ref[half * tile:(half + 1) * tile, head * head_dim:(head + 1) * head_dim]
        scores = [jnp.dot(q_rows, k_scr[p, :, start:start + size], preferred_element_type=F32) for p, start, size in parts_of(half, piece_id)]
        scores[-1] = jnp.where(col_ix <= row_ix, scores[-1], -jnp.inf)
        return scores

    def finish(head, half, piece_id, scores):
        peak = jnp.max(scores[0], axis=-1, keepdims=True)
        for part in scores[1:]:
            peak = jnp.maximum(peak, jnp.max(part, axis=-1, keepdims=True))
        peak = peak * exp_scale
        total = jnp.zeros((tile, 1), F32)
        acc = jnp.zeros((tile, head_dim), F32)
        for part, (p, start, size) in zip(scores, parts_of(half, piece_id)):
            weights = jnp.exp2(part * exp_scale - peak)
            total = total + jnp.sum(weights, axis=-1, keepdims=True)
            acc = acc + jnp.dot(weights.astype(BF16), v_scr[p, start:start + size, :], preferred_element_type=F32)
        o_ref[half * tile:(half + 1) * tile, head * head_dim:(head + 1) * head_dim] = (acc / total).astype(BF16)

    tiles = [(head, half) for head in range(heads_step) for half in range(2)]
    for piece_id in range(n_pieces):
        @pl.when(ids_ref[0] == piece_id)
        def _():
            ahead = scores_of(*tiles[0], piece_id)
            for now, later in zip(tiles, tiles[1:] + [None]):
                scores = ahead
                if later is not None:
                    ahead = scores_of(*later, piece_id)
                finish(*now, piece_id, scores)


def attend(q_rows, kv_list, ids, head_dim):
    piece, width = q_rows.shape
    heads = width // head_dim
    heads_step = 2
    n_pieces = len(kv_list)
    kv_spec = pl.BlockSpec((piece, 2 * head_dim), lambda h, s: (0, 0))
    head_spec = pl.BlockSpec((piece, heads_step * head_dim), lambda h, s: (0, h))
    work = 5 * piece * piece * heads // 2
    return pl.pallas_call(
        functools.partial(attend_kernel, n_pieces=n_pieces, piece=piece, head_dim=head_dim, heads_step=heads_step),
        out_shape=jax.ShapeDtypeStruct((piece, width), BF16),
        grid_spec=pltpu.PrefetchScalarGridSpec(
            num_scalar_prefetch=1,
            grid=(heads // heads_step,),
            in_specs=[head_spec] + [kv_spec] * n_pieces,
            out_specs=head_spec,
            scratch_shapes=[pltpu.VMEM((n_pieces, head_dim, piece), BF16), pltpu.VMEM((n_pieces, piece, head_dim), BF16)],
        ),
        compiler_params=pltpu.CompilerParams(dimension_semantics=('arbitrary',)),
        cost_estimate=pl.CostEstimate(flops=4 * work * head_dim * 2, bytes_accessed=4 * piece * width + 4 * n_pieces * piece * head_dim, transcendentals=work),
        name='attend',
    )(ids, q_rows, *kv_list)


def combine_kernel(slot_ref, gate_ref, base_ref, *refs, n_back, first_slot, capacity):
    back_refs = refs[:n_back]
    out_ref, hot_scr, back_scr = refs[-3:]
    tokens = base_ref.shape[0]

    @pl.when(pl.program_id(0) == 0)
    def _():
        slot_ix = lax.broadcasted_iota(jnp.int32, (2 * tokens, n_back * capacity), 1) + first_slot
        hot_scr[...] = jnp.where(slot_ix == slot_ref[...], 1.0, 0.0).astype(BF16)

    for i in range(n_back):
        back_scr[i * capacity:(i + 1) * capacity, :] = back_refs[i][...]
    picked = jnp.dot(hot_scr[...], back_scr[...], preferred_element_type=F32)
    gated = gate_ref[:, 0:1] * picked[:tokens] + gate_ref[:, 1:2] * picked[tokens:]
    out_ref[...] = (base_ref[...].astype(F32) + gated).astype(out_ref.dtype).reshape(out_ref.shape)


def combine(slots, gates, base, back_list, first, seq=None, n_seq=None, out_prev=None):
    tokens, hidden = base.shape
    n_back = len(back_list)
    capacity = back_list[0].shape[0]
    width = 1024
    whole = lambda shape: pl.BlockSpec(shape, lambda i: (0, 0))
    column = lambda rows: pl.BlockSpec((rows, width), lambda i: (0, i))
    in_specs = [whole((2 * tokens, 1)), whole((tokens, 2)), column(tokens)] + [column(capacity)] * n_back
    args = [slots, gates, base] + list(back_list)
    if out_prev is not None:
        in_specs.append(pl.BlockSpec(memory_space=pl.ANY))
        args.append(out_prev)
    if seq is None:
        out_shape, out_specs = jax.ShapeDtypeStruct((tokens, hidden), F32), column(tokens)
    else:
        out_shape = jax.ShapeDtypeStruct((n_seq, tokens, hidden), BF16)
        out_specs = pl.BlockSpec((1, tokens, width), lambda i: (seq, 0, i))
    return pl.pallas_call(
        functools.partial(combine_kernel, n_back=n_back, first_slot=first * capacity, capacity=capacity),
        out_shape=out_shape,
        grid=(hidden // width,),
        in_specs=in_specs,
        out_specs=out_specs,
        scratch_shapes=[pltpu.VMEM((2 * tokens, n_back * capacity), BF16), pltpu.VMEM((n_back * capacity, width), BF16)],
        input_output_aliases={len(args) - 1: 0} if out_prev is not None else {},
        compiler_params=pltpu.CompilerParams(dimension_semantics=('arbitrary',)),
        cost_estimate=pl.CostEstimate(flops=4 * tokens * n_back * capacity * hidden, bytes_accessed=2 * hidden * (n_back * capacity + 3 * tokens), transcendentals=0),
        name='combine',
    )(*args)


def rank_in_expert(token_hits):
    tokens = token_hits.shape[-2]
    earlier = (jnp.arange(tokens)[None, :] < jnp.arange(tokens)[:, None]).astype(BF16)
    return jnp.einsum('ts,...se->...te', earlier, token_hits.astype(BF16), preferred_element_type=F32).astype(jnp.int32)


def solution(mesh):
    cp_size = mesh.shape['cp']
    tp_size = mesh.shape['tp']
    experts = cp_size * tp_size
    row_spec = P(None, ('data', 'cp', 'tp'), None)
    head_spec = P(None, 'tp', None)
    out_spec = P('tp', None, None)
    expert_spec = P(('cp', 'tp'), None, None)
    both = ('cp', 'tp')
    cores = [[0, 1], [2, 3]]

    def cross_x(rows):
        return lax.ppermute(rows, 'tp', [(t, t ^ 2) for t in range(tp_size)])

    def cross_y(rows):
        return lax.ppermute(rows, 'cp', [(c, c ^ 1) for c in range(cp_size)])

    def pair(rows):
        return lax.all_gather(rows, 'tp', axis=0, tiled=True, axis_index_groups=cores)

    def exchange(rows, k):
        return rows if k == 0 else lax.ppermute(rows, both, [(i, i ^ k) for i in range(experts)])

    def device_step(act_in, route_ids, route_gates, w_query, w_key, w_value, w_out, w_gate, w_up, w_down):
        n_seq, tokens, hidden = act_in.shape
        head_dim = w_query.shape[2]
        capacity = (4 * tokens) // experts
        cp_rank = lax.axis_index('cp')
        tp_rank = lax.axis_index('tp')
        x_rank, core = tp_rank // 2, tp_rank % 2
        me = cp_rank * tp_size + tp_rank
        w_q = w_query.reshape(hidden, -1)
        w_kv = jnp.concatenate([w_key.reshape(hidden, -1), w_value.reshape(hidden, -1)], axis=1)
        w_o = w_out.reshape(-1, hidden)

        piece_of = lambda c, x: jnp.where(x == 0, c, 2 * cp_size - 1 - c)
        piece_ids = [piece_of(cp_rank, x_rank), piece_of(cp_rank, 1 - x_rank), piece_of(1 - cp_rank, x_rank), piece_of(1 - cp_rank, 1 - x_rank)]
        ids_here = jnp.stack([piece_ids[0]] + piece_ids)
        ids_there = jnp.stack([piece_ids[1]] + piece_ids)

        def project(rows):
            kv = jnp.dot(rows, w_kv, preferred_element_type=F32).astype(BF16)
            return kv, jnp.dot(rows, w_q, preferred_element_type=F32).astype(BF16)

        def project_out(rows):
            part = jnp.dot(rows, w_o, preferred_element_type=F32)
            return lax.psum_scatter(part, 'tp', scatter_dimension=0, tiled=True, axis_index_groups=cores)

        ids_by = jnp.stack([route_ids, exchange(route_ids, 1)])
        ids_by = jnp.concatenate([ids_by, cross_x(ids_by)])
        ids_by = jnp.concatenate([ids_by, cross_y(ids_by)])

        hit_here = jnp.any(ids_by == me, axis=-1)
        rank_here = rank_in_expert(hit_here[..., None])[..., 0]
        slot_of = jnp.where(hit_here, rank_here, -1).reshape(experts // 2, 2, n_seq, tokens)
        slot_of = jnp.where(core == 0, slot_of, slot_of[:, ::-1])
        slot_of = jnp.swapaxes(slot_of, 1, 2).reshape(experts // 2, n_seq, 1, 2 * tokens)
        slot_ix = jnp.arange(2 * capacity)[:, None]
        same = jnp.arange(2 * tokens)[None, :] // tokens == (slot_ix // capacity ^ core)
        pick_in = ((slot_of == slot_ix % capacity) & same).astype(BF16)

        hits = route_ids[..., None] == jnp.arange(experts)
        ranks = rank_in_expert(jnp.any(hits, axis=2))
        choice_rank = jnp.sum(hits * ranks[:, :, None, :], axis=-1)
        choice_slot = (route_ids ^ me) * capacity + choice_rank
        choice_slot = jnp.swapaxes(choice_slot, 1, 2).reshape(n_seq, 2 * tokens, 1)

        mids, mids_x, mids_y = [], [], []
        for seq in range(n_seq):
            x_own = act_in[seq]
            x_over = cross_x(x_own)
            rows_here = pair(x_own)
            kv_here, q_here = project(rows_here)
            kv_y_here = cross_y(kv_here)
            rows_there = pair(x_over)
            kv_there, q_there = project(rows_there)
            kv_y_there = cross_y(kv_there)
            kv_list = [kv_here, kv_there, kv_y_here, kv_y_there]
            attn_there = attend(q_there, kv_list, ids_there, head_dim)
            sum_there = project_out(attn_there)
            attn_here = attend(q_here, kv_list, ids_here, head_dim)
            sum_over = cross_x(sum_there)
            sum_here = project_out(attn_here)
            if seq > 0:
                x_own, _ = lax.optimization_barrier((x_own, mids[-1]))
            mids.append((x_own.astype(F32) + (sum_here + sum_over)).astype(BF16))
            mids_x.append(cross_x(mids[-1]))
            mids_y.append(cross_y(mids[-1]))

        out = None
        for seq in range(n_seq):
            mid_diag = cross_y(mids_x[seq])
            rows_of = [mids[seq], mids_x[seq], mids_y[seq], mid_diag]
            backs = [None] * experts
            for group in ((1, 2), (3, 0)):
                picks = []
                for kc in group:
                    rows_two = pair(rows_of[kc])
                    picks.append(jnp.dot(pick_in[kc, seq], rows_two, preferred_element_type=F32).astype(BF16))
                expert_in = jnp.concatenate(picks, axis=0)
                gate_act = jnp.dot(expert_in, w_gate[0], preferred_element_type=F32)
                up_act = jnp.dot(expert_in, w_up[0], preferred_element_type=F32)
                mixed_act = (jax.nn.silu(gate_act) * up_act).astype(BF16)
                mixed_act = lax.optimization_barrier(mixed_act)
                expert_out = jnp.dot(mixed_act, w_down[0], preferred_element_type=F32).astype(BF16)
                for i, kc in enumerate(group):
                    for r in range(2):
                        start = (2 * i + r) * capacity
                        backs[2 * kc + r] = exchange(expert_out[start:start + capacity], 2 * kc + r)
            base, first = mids[seq], 0
            if seq == n_seq - 1:
                first = experts // 2
                base = combine(choice_slot[seq], route_gates[seq], base, backs[:first], 0)
            out = combine(choice_slot[seq], route_gates[seq], base, backs[first:], first, seq, n_seq, out)
        return out

    return jax.shard_map(device_step, mesh=mesh, in_specs=(row_spec, row_spec, row_spec, head_spec, head_spec, head_spec, out_spec, expert_spec, expert_spec, expert_spec), out_specs=row_spec, check_vma=False)
```
